256 devices in a mesh: seq: 32 (over z, y), head: 8 (over x, core).
Axes of the slice: x: 4, y: 4, z: 8, core: 2. Of those that a mesh axis runs over, the one named last changes fastest.
Arguments:
- queries: bfloat16 [32768, 12288], P(('seq', 'head')), may hold values from -8 to 8
- latent: bfloat16 [32768, 512], P(('seq', 'head')), may hold values from -6 to 6
- rope_keys: bfloat16 [32768, 64], P(('seq', 'head')), may hold values from -8 to 8
- key_weight: bfloat16 [512, 8192], P('seq', 'head'), may hold values from -0.25 to 0.25
- value_weight: bfloat16 [512, 8192], P('seq', 'head'), may hold values from -0.25 to 0.25
- doc_lengths: int32 [128], replicated, may hold values from 1 to 510, as said below
Outputs:
- attended: bfloat16 [32768, 8192], P(('seq', 'head'))
The draws below stay inside these ranges and needn't reach their ends.
Inputs may be any that keep to these rules, and one draw needn't show every extreme that they name: `doc_lengths`: the documents lie in order in the pack and their lengths sum to 32768; document 0 starts at position 0 and every other document d starts strictly inside positions d * 256 to (d + 1) * 256 - 1, excluding the first of these; one length is exactly 510.
All inputs are finite; a program needn't handle non-finite values.
Results may differ from the reference program's by a relative error of at most 0.0062.
Values may be sent and summed in bfloat16 or wider, within the bound.
No kernel may reach another device: no remote copies, remote signals or barrier semaphores. Data moves between devices by JAX's collectives and lax.ppermute only.
A program may use at most 64 MiB of HBM per device.

```python
import math
import jax
import jax.numpy as jnp
from jax import lax

KV_RANK = 512
NOPE = 128
ROPE = 64
VDIM = 128
HEADS = 64
TOK_DEV = 128
TOKENS = 32768
DOCS = 128
N_HEAD = 8


def draw_queries(key, part):
    shape = (TOKENS, HEADS, NOPE + ROPE)
    own_key = jax.random.fold_in(key, 11)
    drawn = jnp.clip(2.0 * jax.random.normal(own_key, shape, jnp.float32), -8.0, 8.0)
    return drawn.reshape(TOKENS, HEADS * (NOPE + ROPE)).astype(jnp.bfloat16)


def draw_rope_keys(key, part):
    shape = (TOKENS, ROPE)
    own_key = jax.random.fold_in(key, 12)
    drawn = jnp.clip(jax.random.normal(own_key, shape, jnp.float32), -8.0, 8.0)
    return drawn.astype(jnp.bfloat16)


def draw_doc_lengths(key, part):
    slot_rows = TOKENS // DOCS
    jitter = jax.random.randint(jax.random.fold_in(key, 21), (DOCS,), 1, slot_rows)
    chosen = jax.random.randint(jax.random.fold_in(key, 22), (), 1, DOCS - 1)
    index = jnp.arange(DOCS, dtype=jnp.int32)
    jitter = jnp.where(index == 1, jnp.minimum(jitter, slot_rows - 2), jitter)
    jitter = jnp.where(index == chosen, 1, jitter)
    jitter = jnp.where(index == chosen + 1, slot_rows - 1, jitter)
    jitter = jnp.where(index == 0, 0, jitter)
    starts = index * slot_rows + jitter
    ends = jnp.concatenate([starts[1:], jnp.full((1,), TOKENS, jnp.int32)])
    return (ends - starts).astype(jnp.int32)


def steps_of(key, dims, cuts, low, high):
    factor_of, own = 1.0, jax.random.fold_in(key, 6)
    for position, shards_of in cuts:
        heights = jnp.exp(jax.random.uniform(jax.random.fold_in(own, position), (shards_of,), jnp.float32, low / len(cuts), high / len(cuts)))
        factor_of = factor_of * jnp.repeat(heights, dims[position] // shards_of).reshape([-1 if axis == position else 1 for axis in range(len(dims))])
    return factor_of


def scatter_about(stream_key, extent, spread, bound, pieces=(), held_as=jnp.bfloat16):
    array = spread * jax.random.normal(stream_key, extent, jnp.float32)
    if pieces:
        array = array * steps_of(stream_key, extent, pieces, -0.22, 0.18)
    return jnp.clip(array, -bound, bound).astype(held_as)


def setup_inputs(seed: int = 0) -> dict:
    key_of = jax.random.split(jax.random.key(seed), 7)
    queries = draw_queries(jax.random.fold_in(key_of[6], 71), 0)
    latent = scatter_about(key_of[1], (TOKENS, KV_RANK), 1.0, 6.0, ((0, 256),))
    rope_keys = draw_rope_keys(jax.random.fold_in(key_of[6], 71), 0)
    key_weight = scatter_about(key_of[3], (KV_RANK, HEADS * NOPE), KV_RANK ** -0.5, 0.25, ((0, 32), (1, 8)))
    value_weight = scatter_about(key_of[4], (KV_RANK, HEADS * VDIM), KV_RANK ** -0.5, 0.25, ((0, 32), (1, 8)))
    doc_lengths = draw_doc_lengths(jax.random.fold_in(key_of[6], 71), 0)
    return dict(queries=queries, latent=latent, rope_keys=rope_keys, key_weight=key_weight, value_weight=value_weight, doc_lengths=doc_lengths)


def reference(queries, latent, rope_keys, key_weight, value_weight, doc_lengths):
    total_rows = queries.shape[0]
    group_rows = TOK_DEV * N_HEAD
    block_rows = min(512, group_rows)
    qk_width = NOPE + ROPE
    key_span = group_rows + block_rows
    score_scale = 1.0 / math.sqrt(qk_width)
    starts = (jnp.cumsum(doc_lengths) - doc_lengths).astype(jnp.int32)
    places = jnp.arange(total_rows, dtype=jnp.int32)
    started = (starts[None, :] <= places[:, None]).astype(jnp.int32)
    doc_of = (lax.optimization_barrier(jnp.sum(started, axis=1)) - 1).astype(jnp.int32)
    keys = jnp.dot(latent, key_weight, preferred_element_type=jnp.float32).astype(jnp.bfloat16)
    values = jnp.dot(latent, value_weight, preferred_element_type=jnp.float32).astype(jnp.bfloat16)
    keys_front = jnp.concatenate([jnp.zeros((group_rows, keys.shape[1]), jnp.bfloat16), keys], axis=0)
    values_front = jnp.concatenate([jnp.zeros((group_rows, values.shape[1]), jnp.bfloat16), values], axis=0)
    rope_front = jnp.concatenate([jnp.zeros((group_rows, ROPE), jnp.bfloat16), rope_keys], axis=0)
    docs_front = jnp.concatenate([-jnp.ones((group_rows,), jnp.int32), doc_of], axis=0)

    def one_block(q_index):
        q_start = (q_index * block_rows).astype(jnp.int32)
        q_block = lax.dynamic_slice_in_dim(queries, q_start, block_rows, 0).astype(jnp.float32)
        q_block = q_block.reshape(block_rows, HEADS, qk_width)
        k_nope = lax.dynamic_slice_in_dim(keys_front, q_start, key_span, 0).astype(jnp.float32)
        k_nope = k_nope.reshape(key_span, HEADS, NOPE)
        k_rope = lax.dynamic_slice_in_dim(rope_front, q_start, key_span, 0).astype(jnp.float32)
        k_values = lax.dynamic_slice_in_dim(values_front, q_start, key_span, 0).astype(jnp.float32)
        k_values = k_values.reshape(key_span, HEADS, VDIM)
        q_docs = lax.dynamic_slice_in_dim(doc_of, q_start, block_rows, 0)
        k_docs = lax.dynamic_slice_in_dim(docs_front, q_start, key_span, 0)
        q_places = q_start + jnp.arange(block_rows, dtype=jnp.int32)
        k_places = q_start - group_rows + jnp.arange(key_span, dtype=jnp.int32)
        scores = jnp.einsum('ihd,jhd->hij', q_block[:, :, :NOPE], k_nope)
        scores = (scores + jnp.einsum('ihd,jd->hij', q_block[:, :, NOPE:], k_rope)) * score_scale
        allowed = (q_docs[:, None] == k_docs[None, :]) & (k_places[None, :] <= q_places[:, None])
        scores = jnp.where(allowed[None, :, :], scores, -jnp.inf)
        row_peak = lax.optimization_barrier(jnp.max(scores, axis=2, keepdims=True))
        expo = jnp.exp(scores - row_peak)
        row_sum = lax.optimization_barrier(jnp.sum(expo, axis=2))
        rounded = lax.optimization_barrier(expo.astype(jnp.bfloat16)).astype(jnp.float32)
        mixed = jnp.einsum('hij,jhd->ihd', rounded, k_values) / jnp.transpose(row_sum)[:, :, None]
        return mixed.reshape(block_rows, HEADS * VDIM).astype(jnp.bfloat16)
    attended = lax.map(one_block, jnp.arange(total_rows // block_rows, dtype=jnp.int32))
    return attended.reshape(total_rows, HEADS * VDIM)
```

```python
import functools
import math

import jax
import jax.numpy as jnp
from jax import lax
from jax.experimental import pallas as pl
from jax.experimental.pallas import tpu as pltpu
from jax.sharding import Mesh
from jax.sharding import PartitionSpec as P

NOPE = 128
ROPE = 64
VDIM = 128
WIDE = 256
SEG = 256
HALO = 512
SEQ = ("z", "y")
GROUP = ("x", "c")
EVERY = ("z", "y", "x", "c")
INTERPRET = False
LOWEST = -1e30


def spread(value, axes):
    count = lax.axis_size(axes)
    copies = jnp.broadcast_to(value[None], (count, *value.shape))
    return lax.all_to_all(copies, axes, 0, 0)


def shifted(value, axes, steps):
    count = lax.axis_size(axes)
    return lax.ppermute(value, axes, [(i, i + steps) for i in range(count - steps)])


def keys_kernel(latent_ref, wk_ref, wv_ref, k_ref, v_ref):
    rank = wk_ref.shape[0]
    latent = latent_ref[:, :rank]
    rope = latent_ref[:, rank:].astype(jnp.float32)
    rope_high = pltpu.roll(rope, ROPE, 1)
    low = lax.broadcasted_iota(jnp.int32, rope.shape, 1) < ROPE
    keys = jnp.dot(latent, wk_ref[...], preferred_element_type=jnp.float32)
    turned = pltpu.roll(keys[:, NOPE:], ROPE, 1)
    k_ref[:, 0:128] = keys[:, :NOPE].astype(jnp.bfloat16)
    k_ref[:, 128:256] = rope.astype(jnp.bfloat16)
    k_ref[:, 256:384] = jnp.where(low, 0.0, turned).astype(jnp.bfloat16)
    k_ref[:, 384:512] = jnp.where(low, turned, rope_high).astype(jnp.bfloat16)
    values = jnp.dot(latent, wv_ref[...], preferred_element_type=jnp.float32)
    v_ref[...] = values.astype(jnp.bfloat16)


def project(latent_rows, wk, wv):
    rows, wide = latent_rows.shape
    rank, cols = wk.shape
    pairs = cols // (2 * NOPE)
    block = 512
    return pl.pallas_call(
        keys_kernel,
        grid=(pairs, rows // block),
        in_specs=[
            pl.BlockSpec((block, wide), lambda p, r: (r, 0)),
            pl.BlockSpec((rank, 2 * NOPE), lambda p, r: (0, p)),
            pl.BlockSpec((rank, 2 * VDIM), lambda p, r: (0, p)),
        ],
        out_specs=[
            pl.BlockSpec((block, 2 * WIDE), lambda p, r: (r, p)),
            pl.BlockSpec((block, 2 * VDIM), lambda p, r: (r, p)),
        ],
        out_shape=[
            jax.ShapeDtypeStruct((rows, pairs * 2 * WIDE), jnp.bfloat16),
            jax.ShapeDtypeStruct((rows, pairs * 2 * VDIM), jnp.bfloat16),
        ],
        cost_estimate=pl.CostEstimate(
            flops=4 * rows * rank * cols, bytes_accessed=8 * rows * cols, transcendentals=0
        ),
        interpret=INTERPRET,
        name="project",
    )(latent_rows, wk, wv)


def attend_kernel(score_scale, q_ref, k_ref, v_ref, start_ref, o_ref):
    seg = pl.program_id(1)
    window = SEG + HALO
    first = pl.multiple_of(seg * SEG, SEG)
    row = lax.broadcasted_iota(jnp.int32, (SEG, window), 0)
    col = lax.broadcasted_iota(jnp.int32, (SEG, window), 1)
    allowed = (col <= row + HALO) & (col >= start_ref[...] - first)
    bias = jnp.where(allowed, 0.0, LOWEST)
    for half in range(2):
        q = q_ref[:, 128 * half : 128 * half + WIDE]
        k = k_ref[pl.ds(first, window), WIDE * half : WIDE * (half + 1)]
        scores = lax.dot_general(
            q, k, (((1,), (1,)), ((), ())), preferred_element_type=jnp.float32
        )
        scores = scores * score_scale + bias
        peak = jnp.max(scores, axis=1, keepdims=True)
        expo = jnp.exp2(scores - peak)
        total = jnp.sum(expo, axis=1, keepdims=True)
        v = v_ref[pl.ds(first, window), VDIM * half : VDIM * (half + 1)]
        mixed = jnp.dot(expo.astype(jnp.bfloat16), v, preferred_element_type=jnp.float32)
        o_ref[:, VDIM * half : VDIM * (half + 1)] = (mixed / total).astype(jnp.bfloat16)


def attend(queries, keys, values, starts):
    rows = queries.shape[0]
    heads = values.shape[1] // VDIM
    segs = rows // SEG
    span = keys.shape[0]
    score_scale = math.log2(math.e) / math.sqrt(NOPE + ROPE)
    return pl.pallas_call(
        functools.partial(attend_kernel, score_scale),
        grid=(heads // 2, segs),
        in_specs=[
            pl.BlockSpec((SEG, 2 * (NOPE + ROPE)), lambda p, s: (s, p)),
            pl.BlockSpec((span, 2 * WIDE), lambda p, s: (0, p)),
            pl.BlockSpec((span, 2 * VDIM), lambda p, s: (0, p)),
            pl.BlockSpec((SEG, 1), lambda p, s: (s, 0)),
        ],
        out_specs=pl.BlockSpec((SEG, 2 * VDIM), lambda p, s: (s, p)),
        out_shape=jax.ShapeDtypeStruct((rows, heads * VDIM), jnp.bfloat16),
        cost_estimate=pl.CostEstimate(
            flops=2 * heads * rows * (SEG + HALO) * (WIDE + VDIM),
            bytes_accessed=2 * rows * heads * 1024,
            transcendentals=heads * rows * (SEG + HALO),
        ),
        interpret=INTERPRET,
        name="attend",
    )(queries, keys, values, starts)


def shards(queries, latent, rope_keys, key_weight, value_weight, doc_lengths):
    tok_rows, rank = latent.shape
    groups = lax.axis_size(GROUP)
    group_rows = tok_rows * groups
    local_width = queries.shape[1] // groups
    local_cols = key_weight.shape[1]

    by_heads = jnp.stack(
        [queries[:, g * local_width : (g + 1) * local_width] for g in range(groups)]
    )
    my_queries = lax.all_to_all(by_heads, GROUP, 0, 0).reshape(group_rows, local_width)

    both = jnp.concatenate([latent, rope_keys], axis=1)
    group_latent = spread(both, GROUP).reshape(group_rows, rank + ROPE)
    halo = shifted(group_latent[group_rows - HALO :], SEQ, 1)
    latent_rows = jnp.concatenate([halo, group_latent], axis=0)
    latent_rows = jnp.pad(latent_rows, ((0, 0), (0, 128 - ROPE)))

    weights = jnp.concatenate([key_weight, value_weight], axis=1)
    over_z = spread(weights, "z")
    over_y = spread(over_z, "y")
    whole = jnp.transpose(over_y, (1, 0, 2, 3)).reshape(rank, 2 * local_cols)
    wk, wv = whole[:, :local_cols], whole[:, local_cols:]

    docs = doc_lengths.shape[0]
    before = jnp.arange(docs)[None, :] < jnp.arange(docs)[:, None]
    starts = jnp.sum(jnp.where(before, doc_lengths[None, :], 0), axis=1)
    first_place = lax.axis_index(SEQ) * group_rows
    places = first_place + jnp.arange(group_rows, dtype=jnp.int32)
    own = jnp.max(
        jnp.where(starts[None, :] <= places[:, None], starts[None, :], 0), axis=1, keepdims=True
    )
    own = (own - first_place + HALO).astype(jnp.int32)

    keys, values = project(latent_rows, wk, wv)
    attended = attend(my_queries, keys, values, own)
    back = lax.all_to_all(attended.reshape(groups, tok_rows, -1), GROUP, 0, 0)
    return jnp.concatenate([back[g] for g in range(groups)], axis=1)


def solution(mesh):
    y = 4 if mesh.shape["seq"] % 4 == 0 else 1
    torus = Mesh(mesh.devices.reshape(-1, y, mesh.shape["head"] // 2, 2), EVERY)
    in_specs = (
        P(EVERY, None),
        P(EVERY, None),
        P(EVERY, None),
        P(SEQ, GROUP),
        P(SEQ, GROUP),
        P(),
    )
    return jax.shard_map(
        shards, mesh=torus, in_specs=in_specs, out_specs=P(EVERY, None), check_vma=False
    )
```

```python
import functools
import math

import jax
import jax.numpy as jnp
from jax import lax
from jax.experimental import pallas as pl
from jax.experimental.pallas import tpu as pltpu
from jax.sharding import Mesh
from jax.sharding import PartitionSpec as P


NOPE = 128
ROPE = 64
VDIM = 128
WIDE = 256
SUB = 128
HALO = 512
SEQ = ("z", "y")
GROUP = ("x", "c")
EVERY = ("z", "y", "x", "c")
CHUNK = 512
STRIP = 16
VMEM_LIMIT = 24 * 2**20
INTERPRET = False
LOWEST = -1e30


def spread(value, axis):
    count = lax.axis_size(axis)
    copies = jnp.broadcast_to(value[None], (count, *value.shape))
    return lax.all_to_all(copies, axis, 0, 0)


def shifted(value, axes, steps):
    count = lax.axis_size(axes)
    return lax.ppermute(value, axes, [(i, i + steps) for i in range(count - steps)])


def turned(value, axis, steps):
    count = lax.axis_size(axis)
    return lax.ppermute(value, axis, [(i, (i + steps) % count) for i in range(count)])


def swapped(value):
    return lax.ppermute(value, "c", [(0, 1), (1, 0)])


def hops(step, flip):
    chips = lax.axis_size("x")
    return [
        (2 * x + c, 2 * ((x + step) % chips) + (c ^ flip)) for x in range(chips) for c in range(2)
    ]


def project_kernel(weight_rows, chips, at_ref, mine_ref, other_ref, *refs):
    weights, (k_ref, v_ref, w_ref, l_ref) = refs[:-4], refs[-4:]
    over_y = len(weights)
    for step, piece in enumerate(weights):
        at_y = lax.rem(at_ref[1] + over_y - step, over_y)
        for z in range(piece.shape[0] // weight_rows):
            at = pl.multiple_of((z * over_y + at_y) * weight_rows, weight_rows)
            w_ref[pl.ds(at, weight_rows), :] = piece[z * weight_rows : (z + 1) * weight_rows, :]
    rank = w_ref.shape[0]
    cols = v_ref.shape[1]
    for part, core in ((mine_ref, at_ref[2]), (other_ref, 1 - at_ref[2])):
        for i in range(part.shape[0] // SUB):
            chip = lax.rem(at_ref[0] + chips - i, chips) if i < chips else i - chips
            first = HALO if i < chips else 0
            at = pl.multiple_of(first + (2 * chip + core) * SUB, SUB)
            l_ref[pl.ds(at, SUB), :] = part[i * SUB : (i + 1) * SUB, :]

    for at in range(0, l_ref.shape[0], CHUNK):
        rows = slice(at, at + CHUNK)
        rope = l_ref[rows, rank:].astype(jnp.float32)
        rope_high = pltpu.roll(rope, ROPE, 1)
        low = lax.broadcasted_iota(jnp.int32, rope.shape, 1) < ROPE
        for col in range(0, 2 * cols, 256):
            product = jnp.dot(
                l_ref[rows, :rank], w_ref[:, col : col + 256], preferred_element_type=jnp.float32
            )
            if col >= cols:
                v_ref[rows, col - cols : col - cols + 256] = product.astype(jnp.bfloat16)
                continue
            moved = pltpu.roll(product[:, NOPE:], ROPE, 1)
            out = 2 * col
            k_ref[rows, out : out + 128] = product[:, :NOPE].astype(jnp.bfloat16)
            k_ref[rows, out + 128 : out + 256] = l_ref[rows, rank:]
            k_ref[rows, out + 256 : out + 384] = jnp.where(low, 0.0, moved).astype(jnp.bfloat16)
            k_ref[rows, out + 384 : out + 512] = jnp.where(low, moved, rope_high).astype(
                jnp.bfloat16
            )


IN_VMEM = pl.BlockSpec(memory_space=pltpu.VMEM)
IN_SMEM = pl.BlockSpec(memory_space=pltpu.SMEM)


def project(mine, other, weights):
    chips, over_y = lax.axis_size("x"), len(weights)
    rows = mine.shape[0] * 2
    cols = weights[0].shape[1] // 2
    rank = weights[0].shape[0] * over_y
    at = jnp.stack([lax.axis_index(axis) for axis in ("x", "y", "c")]).astype(jnp.int32)
    weight_rows = weights[0].shape[0] // lax.axis_size("z")
    return pl.pallas_call(
        functools.partial(project_kernel, weight_rows, chips),
        in_specs=[IN_SMEM] + [IN_VMEM] * (2 + over_y),
        out_specs=[IN_VMEM, IN_VMEM],
        scratch_shapes=[
            pltpu.VMEM((rank, 2 * cols), jnp.bfloat16),
            pltpu.VMEM((rows, mine.shape[1]), jnp.bfloat16),
        ],
        out_shape=[
            jax.ShapeDtypeStruct((rows, 2 * cols), jnp.bfloat16),
            jax.ShapeDtypeStruct((rows, cols), jnp.bfloat16),
        ],
        compiler_params=pltpu.CompilerParams(vmem_limit_bytes=VMEM_LIMIT),
        cost_estimate=pl.CostEstimate(
            flops=4 * rows * rank * cols, bytes_accessed=8 * rows * cols, transcendentals=0
        ),
        interpret=INTERPRET,
        name="project",
    )(at, mine, other, *weights)


def attend_kernel(
    score_scale, at_ref, q0_ref, q1_ref, k_ref, v_ref, start_ref, o0_ref, o1_ref, *scratch
):
    q_ref, o_ref, bias_ref, s_ref, p_ref, t_ref = scratch
    rows, window = 2 * SUB, 2 * SUB + HALO
    heads = v_ref.shape[1] // VDIM
    base = pl.multiple_of(at_ref[0], 2 * SUB)
    places = [pl.ds(pl.multiple_of(at_ref[1 + i], SUB), SUB) for i in range(2)]
    q_ref[places[0], :] = q0_ref[...]
    q_ref[places[1], :] = q1_ref[...]
    for at in range(0, rows, STRIP):
        row = lax.broadcasted_iota(jnp.int32, (STRIP, window), 0) + at
        col = lax.broadcasted_iota(jnp.int32, (STRIP, window), 1)
        start = start_ref[pl.ds(pl.multiple_of(base + at, STRIP), STRIP), :] - base
        allowed = (col <= row + HALO) & (col >= start)
        bias_ref[at : at + STRIP, :] = jnp.where(allowed, 0.0, LOWEST)
    span = pl.ds(base, window)

    @pl.loop(0, heads // 2)
    def _(pair):
        for half in range(2):
            q_at = pl.multiple_of(pair * 2 * (NOPE + ROPE) + 128 * half, 128)
            v_at = pl.ds(pl.multiple_of((2 * pair + half) * VDIM, VDIM), VDIM)
            k_at = pl.ds(pl.multiple_of((2 * pair + half) * WIDE, WIDE), WIDE)
            s_ref[half] = lax.dot_general(
                q_ref[:, pl.ds(q_at, WIDE)],
                k_ref[span, k_at],
                (((1,), (1,)), ((), ())),
                preferred_element_type=jnp.float32,
            )
        for half in range(2):
            v_at = pl.ds(pl.multiple_of((2 * pair + half) * VDIM, VDIM), VDIM)
            for at in range(0, rows, STRIP):
                part = slice(at, at + STRIP)
                scores = s_ref[half, part, :] * score_scale + bias_ref[part, :]
                expo = jnp.exp2(scores - jnp.max(scores, axis=1, keepdims=True))
                t_ref[half, part, :] = jnp.broadcast_to(
                    jnp.sum(expo, axis=1, keepdims=True), (STRIP, VDIM)
                )
                p_ref[half, part, :] = expo.astype(jnp.bfloat16)
            mixed = jnp.dot(p_ref[half], v_ref[span, v_at], preferred_element_type=jnp.float32)
            o_ref[:, v_at] = (mixed / t_ref[half]).astype(jnp.bfloat16)

    o0_ref[...] = o_ref[places[0], :]
    o1_ref[...] = o_ref[places[1], :]


def attend(chip, mine, other, keys, values, starts):
    rows, width = mine.shape
    heads = values.shape[1] // VDIM
    window = 2 * SUB + HALO
    core = lax.axis_index("c")
    at = jnp.stack([chip * 2 * SUB, core * SUB, (1 - core) * SUB]).astype(jnp.int32)
    score_scale = math.log2(math.e) / math.sqrt(NOPE + ROPE)
    o_shape = jax.ShapeDtypeStruct((rows, heads * VDIM), jnp.bfloat16)
    return pl.pallas_call(
        functools.partial(attend_kernel, score_scale),
        in_specs=[IN_SMEM] + [IN_VMEM] * 5,
        out_specs=[IN_VMEM, IN_VMEM],
        out_shape=[o_shape, o_shape],
        scratch_shapes=[
            pltpu.VMEM((2 * SUB, width), jnp.bfloat16),
            pltpu.VMEM((2 * SUB, heads * VDIM), jnp.bfloat16),
            pltpu.VMEM((2 * SUB, window), jnp.float32),
            pltpu.VMEM((2, 2 * SUB, window), jnp.float32),
            pltpu.VMEM((2, 2 * SUB, window), jnp.bfloat16),
            pltpu.VMEM((2, 2 * SUB, VDIM), jnp.float32),
        ],
        compiler_params=pltpu.CompilerParams(vmem_limit_bytes=VMEM_LIMIT),
        cost_estimate=pl.CostEstimate(
            flops=4 * heads * rows * window * (WIDE + VDIM),
            bytes_accessed=4 * rows * heads * 1024,
            transcendentals=2 * heads * rows * window,
        ),
        interpret=INTERPRET,
        name="attend",
    )(at, mine, other, keys, values, starts)


def whole(queries, latent, rope_keys, key_weight, value_weight, doc_lengths):
    tok_rows, _ = latent.shape
    chips = lax.axis_size("x")
    groups = 2 * chips
    group_rows = tok_rows * groups
    width = queries.shape[1] // groups
    x, core = lax.axis_index("x"), lax.axis_index("c")

    def block_of(step, flip):
        return 2 * lax.rem(x + step, chips) + (core ^ flip)

    weights = jnp.concatenate([key_weight, value_weight], axis=1)
    weights = spread(weights, "z").reshape(-1, weights.shape[1])
    over_y = lax.axis_size("y")
    weight_pieces = [weights] + [turned(weights, "y", s) for s in range(1, over_y)]

    both = jnp.concatenate(
        [latent, rope_keys, jnp.zeros((tok_rows, 128 - ROPE), jnp.bfloat16)], axis=1
    )
    parts = [both] + [turned(both, "x", s) for s in range(1, chips)]
    halo_chips = HALO // (2 * tok_rows)
    last = []
    for chip in range(chips - halo_chips, chips):
        behind = lax.rem(x + chips - chip, chips)
        last.append(lax.select_n(behind, *parts))
    last = jnp.concatenate(last, axis=0)
    earlier = shifted(last, SEQ, 1)
    mine = jnp.concatenate([*lax.optimization_barrier(parts), earlier], axis=0)
    other = swapped(mine)

    def sent(step, flip):
        out = lax.dynamic_slice_in_dim(queries, width * block_of(step, flip), width, 1)
        if not (step or flip):
            return out
        return lax.ppermute(out, GROUP, hops(step, flip))

    arrived = {(s, f): sent(s, f) for s in range(chips) for f in (0, 1)}

    docs = doc_lengths.shape[0]
    earlier = jnp.arange(docs)[None, :] < jnp.arange(docs)[:, None]
    starts = jnp.sum(jnp.where(earlier, doc_lengths[None, :], 0), axis=1)
    first_place = lax.axis_index(SEQ) * group_rows
    places = first_place + jnp.arange(group_rows, dtype=jnp.int32)
    own = jnp.max(
        jnp.where(starts[None, :] <= places[:, None], starts[None, :], 0), axis=1, keepdims=True
    )
    own = (own - first_place + HALO).astype(jnp.int32)

    keys, values = project(mine, other, weight_pieces)

    result = jnp.zeros((tok_rows, groups * value_weight.shape[1]), jnp.bfloat16)
    for step in (1, 3, 2, 0):
        chip = lax.rem(x + chips - step, chips)
        pair = attend(chip, arrived[step, 0], arrived[step, 1], keys, values, own)
        for flip in (0, 1):
            back = pair[flip]
            if step or flip:
                back = lax.ppermute(back, GROUP, [(b, a) for a, b in hops(step, flip)])
            at = value_weight.shape[1] * block_of(step, flip)
            result = lax.dynamic_update_slice(result, back, (0, at))
    return result


def solution(mesh):
    y = 4 if mesh.shape["seq"] % 4 == 0 else 1
    torus = Mesh(mesh.devices.reshape(-1, y, mesh.shape["head"] // 2, 2), EVERY)
    in_specs = (
        P(EVERY, None),
        P(EVERY, None),
        P(EVERY, None),
        P(SEQ, GROUP),
        P(SEQ, GROUP),
        P(),
    )
    return jax.shard_map(
        whole, mesh=torus, in_specs=in_specs, out_specs=P(EVERY, None), check_vma=False
    )
```

```python
import functools
import math

import jax
import jax.numpy as jnp
from jax import lax
from jax.experimental import pallas as pl
from jax.experimental.pallas import tpu as pltpu
from jax.sharding import Mesh
from jax.sharding import PartitionSpec as P


NOPE = 128
ROPE = 64
VDIM = 128
WIDE = 256
SUB = 128
HALO = 512
SEQ = ("z", "y")
GROUP = ("x", "c")
EVERY = ("z", "y", "x", "c")
CHUNK = 512
STRIP = 16
VMEM_LIMIT = 24 * 2**20
INTERPRET = False
LOWEST = -1e30


def spread(value, axis):
    count = lax.axis_size(axis)
    copies = jnp.broadcast_to(value[None], (count, *value.shape))
    return lax.all_to_all(copies, axis, 0, 0)


def shifted(value, axes, steps):
    count = lax.axis_size(axes)
    return lax.ppermute(value, axes, [(i, i + steps) for i in range(count - steps)])


def turned(value, axis, steps):
    count = lax.axis_size(axis)
    return lax.ppermute(value, axis, [(i, (i + steps) % count) for i in range(count)])


def swapped(value):
    return lax.ppermute(value, "c", [(0, 1), (1, 0)])


def hops(step, flip):
    chips = lax.axis_size("x")
    return [
        (2 * x + c, 2 * ((x + step) % chips) + (c ^ flip)) for x in range(chips) for c in range(2)
    ]


def project_kernel(weight_rows, places, chips, at_ref, mine_ref, other_ref, *refs):
    weights, (k_ref, v_ref, w_ref, l_ref) = iter(refs[:-4]), refs[-4:]
    over_y = len(places)
    for step, parts in places:
        at_y = lax.rem(at_ref[1] + over_y - step, over_y)
        z = 0
        for _ in range(parts):
            piece = next(weights)
            for row in range(0, piece.shape[0], weight_rows):
                at = pl.multiple_of((z * over_y + at_y) * weight_rows, weight_rows)
                w_ref[pl.ds(at, weight_rows), :] = piece[row : row + weight_rows, :]
                z += 1
    rank = w_ref.shape[0]
    cols = v_ref.shape[1]
    for part, core in ((mine_ref, at_ref[2]), (other_ref, 1 - at_ref[2])):
        for i in range(part.shape[0] // SUB):
            chip = lax.rem(at_ref[0] + chips - i, chips) if i < chips else i - chips
            first = HALO if i < chips else 0
            at = pl.multiple_of(first + (2 * chip + core) * SUB, SUB)
            l_ref[pl.ds(at, SUB), :] = part[i * SUB : (i + 1) * SUB, :]

    for at in range(0, l_ref.shape[0], CHUNK):
        rows = slice(at, at + CHUNK)
        rope = l_ref[rows, rank:].astype(jnp.float32)
        rope_high = pltpu.roll(rope, ROPE, 1)
        low = lax.broadcasted_iota(jnp.int32, rope.shape, 1) < ROPE
        for col in range(0, 2 * cols, 256):
            product = jnp.dot(
                l_ref[rows, :rank], w_ref[:, col : col + 256], preferred_element_type=jnp.float32
            )
            if col >= cols:
                v_ref[rows, col - cols : col - cols + 256] = product.astype(jnp.bfloat16)
                continue
            moved = pltpu.roll(product[:, NOPE:], ROPE, 1)
            out = 2 * col
            k_ref[rows, out : out + 128] = product[:, :NOPE].astype(jnp.bfloat16)
            k_ref[rows, out + 128 : out + 256] = l_ref[rows, rank:]
            k_ref[rows, out + 256 : out + 384] = jnp.where(low, 0.0, moved).astype(jnp.bfloat16)
            k_ref[rows, out + 384 : out + 512] = jnp.where(low, moved, rope_high).astype(
                jnp.bfloat16
            )


IN_VMEM = pl.BlockSpec(memory_space=pltpu.VMEM)
IN_SMEM = pl.BlockSpec(memory_space=pltpu.SMEM)


def joined_kernel(*refs):
    *parts, out_ref = refs
    at = 0
    for part in parts:
        out_ref[at : at + part.shape[0], :] = part[...]
        at += part.shape[0]


def joined(parts):
    rows = sum(part.shape[0] for part in parts)
    return pl.pallas_call(
        joined_kernel,
        in_specs=[IN_VMEM] * len(parts),
        out_specs=IN_VMEM,
        out_shape=jax.ShapeDtypeStruct((rows, parts[0].shape[1]), parts[0].dtype),
        compiler_params=pltpu.CompilerParams(vmem_limit_bytes=VMEM_LIMIT),
        cost_estimate=pl.CostEstimate(
            flops=rows * 1024, bytes_accessed=rows * 2560, transcendentals=0
        ),
        interpret=INTERPRET,
        name="joined",
    )(*parts)


def project(mine, other, weights):
    chips = lax.axis_size("x")
    rows = mine.shape[0] * 2
    places = tuple((step, len(parts)) for step, *parts in weights)
    weights = [part for _, *parts in weights for part in parts]
    cols = weights[0].shape[1] // 2
    rank = weights[0].shape[0] * len(places)
    at = jnp.stack([lax.axis_index(axis) for axis in ("x", "y", "c")]).astype(jnp.int32)
    weight_rows = weights[0].shape[0] // lax.axis_size("z")
    return pl.pallas_call(
        functools.partial(project_kernel, weight_rows, places, chips),
        in_specs=[IN_SMEM] + [IN_VMEM] * (2 + len(weights)),
        out_specs=[IN_VMEM, IN_VMEM],
        scratch_shapes=[
            pltpu.VMEM((rank, 2 * cols), jnp.bfloat16),
            pltpu.VMEM((rows, mine.shape[1]), jnp.bfloat16),
        ],
        out_shape=[
            jax.ShapeDtypeStruct((rows, 2 * cols), jnp.bfloat16),
            jax.ShapeDtypeStruct((rows, cols), jnp.bfloat16),
        ],
        compiler_params=pltpu.CompilerParams(vmem_limit_bytes=VMEM_LIMIT),
        cost_estimate=pl.CostEstimate(
            flops=4 * rows * rank * cols, bytes_accessed=8 * rows * cols, transcendentals=0
        ),
        interpret=INTERPRET,
        name="project",
    )(at, mine, other, *weights)


def attend_kernel(
    score_scale, at_ref, q0_ref, q1_ref, k_ref, v_ref, start_ref, o0_ref, o1_ref, *scratch
):
    q_ref, o_ref, bias_ref, s_ref, p_ref, t_ref = scratch
    rows, window = 2 * SUB, 2 * SUB + HALO
    heads = v_ref.shape[1] // VDIM
    base = pl.multiple_of(at_ref[0], 2 * SUB)
    places = [pl.ds(pl.multiple_of(at_ref[1 + i], SUB), SUB) for i in range(2)]
    q_ref[places[0], :] = q0_ref[...]
    q_ref[places[1], :] = q1_ref[...]
    for at in range(0, rows, STRIP):
        row = lax.broadcasted_iota(jnp.int32, (STRIP, window), 0) + at
        col = lax.broadcasted_iota(jnp.int32, (STRIP, window), 1)
        start = start_ref[pl.ds(pl.multiple_of(base + at, STRIP), STRIP), :] - base
        allowed = (col <= row + HALO) & (col >= start)
        bias_ref[at : at + STRIP, :] = jnp.where(allowed, 0.0, LOWEST)
    span = pl.ds(base, window)

    @pl.loop(0, heads // 2)
    def _(pair):
        for half in range(2):
            q_at = pl.multiple_of(pair * 2 * (NOPE + ROPE) + 128 * half, 128)
            v_at = pl.ds(pl.multiple_of((2 * pair + half) * VDIM, VDIM), VDIM)
            k_at = pl.ds(pl.multiple_of((2 * pair + half) * WIDE, WIDE), WIDE)
            s_ref[half] = lax.dot_general(
                q_ref[:, pl.ds(q_at, WIDE)],
                k_ref[span, k_at],
                (((1,), (1,)), ((), ())),
                preferred_element_type=jnp.float32,
            )
        for half in range(2):
            v_at = pl.ds(pl.multiple_of((2 * pair + half) * VDIM, VDIM), VDIM)
            for at in range(0, rows, STRIP):
                part = slice(at, at + STRIP)
                scores = s_ref[half, part, :] * score_scale + bias_ref[part, :]
                expo = jnp.exp2(scores - jnp.max(scores, axis=1, keepdims=True))
                t_ref[half, part, :] = jnp.broadcast_to(
                    jnp.sum(expo, axis=1, keepdims=True), (STRIP, VDIM)
                )
                p_ref[half, part, :] = expo.astype(jnp.bfloat16)
            mixed = jnp.dot(p_ref[half], v_ref[span, v_at], preferred_element_type=jnp.float32)
            o_ref[:, v_at] = (mixed / t_ref[half]).astype(jnp.bfloat16)

    o0_ref[...] = o_ref[places[0], :]
    o1_ref[...] = o_ref[places[1], :]


def attend(chip, mine, other, keys, values, starts):
    rows, width = mine.shape
    heads = values.shape[1] // VDIM
    window = 2 * SUB + HALO
    core = lax.axis_index("c")
    at = jnp.stack([chip * 2 * SUB, core * SUB, (1 - core) * SUB]).astype(jnp.int32)
    score_scale = math.log2(math.e) / math.sqrt(NOPE + ROPE)
    o_shape = jax.ShapeDtypeStruct((rows, heads * VDIM), jnp.bfloat16)
    return pl.pallas_call(
        functools.partial(attend_kernel, score_scale),
        in_specs=[IN_SMEM] + [IN_VMEM] * 5,
        out_specs=[IN_VMEM, IN_VMEM],
        out_shape=[o_shape, o_shape],
        scratch_shapes=[
            pltpu.VMEM((2 * SUB, width), jnp.bfloat16),
            pltpu.VMEM((2 * SUB, heads * VDIM), jnp.bfloat16),
            pltpu.VMEM((2 * SUB, window), jnp.float32),
            pltpu.VMEM((2, 2 * SUB, window), jnp.float32),
            pltpu.VMEM((2, 2 * SUB, window), jnp.bfloat16),
            pltpu.VMEM((2, 2 * SUB, VDIM), jnp.float32),
        ],
        compiler_params=pltpu.CompilerParams(vmem_limit_bytes=VMEM_LIMIT),
        cost_estimate=pl.CostEstimate(
            flops=4 * heads * rows * window * (WIDE + VDIM),
            bytes_accessed=4 * rows * heads * 1024,
            transcendentals=2 * heads * rows * window,
        ),
        interpret=INTERPRET,
        name="attend",
    )(at, mine, other, keys, values, starts)


def whole(queries, latent, rope_keys, key_weight, value_weight, doc_lengths):
    tok_rows, _ = latent.shape
    chips = lax.axis_size("x")
    groups = 2 * chips
    group_rows = tok_rows * groups
    width = queries.shape[1] // groups
    x, core = lax.axis_index("x"), lax.axis_index("c")

    def block_of(step, flip):
        return 2 * lax.rem(x + step, chips) + (core ^ flip)

    weights = jnp.concatenate([key_weight, value_weight], axis=1)
    weights = spread(weights, "z").reshape(-1, weights.shape[1])
    over_y = lax.axis_size("y")
    weight_pieces = [(s, turned(weights, "y", s) if s else weights) for s in range(over_y)]

    both = jnp.concatenate(
        [latent, rope_keys, jnp.zeros((tok_rows, 128 - ROPE), jnp.bfloat16)], axis=1
    )
    parts = [both] + [turned(both, "x", s) for s in range(1, chips)]
    halo_chips = HALO // (2 * tok_rows)
    last = []
    for chip in range(chips - halo_chips, chips):
        behind = lax.rem(x + chips - chip, chips)
        last.append(lax.select_n(behind, *parts))
    last = jnp.concatenate(last, axis=0)
    earlier = shifted(last, SEQ, 1)
    mine = joined([*parts, earlier])
    other = swapped(mine)

    late, _ = lax.optimization_barrier((queries, last))

    def sent(step, flip):
        out = lax.dynamic_slice_in_dim(queries if step % 2 else late, width * block_of(step, flip), width, 1)
        if not (step or flip):
            return out
        return lax.ppermute(out, GROUP, hops(step, flip))

    arrived = {(s, f): sent(s, f) for s in range(chips) for f in (0, 1)}

    docs = doc_lengths.shape[0]
    earlier = jnp.arange(docs)[None, :] < jnp.arange(docs)[:, None]
    starts = jnp.sum(jnp.where(earlier, doc_lengths[None, :], 0), axis=1)
    first_place = lax.axis_index(SEQ) * group_rows
    places = first_place + jnp.arange(group_rows, dtype=jnp.int32)
    own = jnp.max(
        jnp.where(starts[None, :] <= places[:, None], starts[None, :], 0), axis=1, keepdims=True
    )
    own = (own - first_place + HALO).astype(jnp.int32)

    keys, values = project(mine, other, weight_pieces)

    result = jnp.zeros((tok_rows, groups * value_weight.shape[1]), jnp.bfloat16)
    for step in (2, 1, 3, 0):
        chip = lax.rem(x + chips - step, chips)
        pair = attend(chip, arrived[step, 0], arrived[step, 1], keys, values, own)
        for flip in (0, 1):
            back = pair[flip]
            if step or flip:
                back = lax.ppermute(back, GROUP, [(b, a) for a, b in hops(step, flip)])
            at = value_weight.shape[1] * block_of(step, flip)
            result = lax.dynamic_update_slice(result, back, (0, at))
    return result


def solution(mesh):
    y = 4 if mesh.shape["seq"] % 4 == 0 else 1
    torus = Mesh(mesh.devices.reshape(-1, y, mesh.shape["head"] // 2, 2), EVERY)
    in_specs = (
        P(EVERY, None),
        P(EVERY, None),
        P(EVERY, None),
        P(SEQ, GROUP),
        P(SEQ, GROUP),
        P(),
    )
    return jax.shard_map(
        whole, mesh=torus, in_specs=in_specs, out_specs=P(EVERY, None), check_vma=False
    )
```

```python
import functools
import math

import jax
import jax.numpy as jnp
from jax import lax
from jax.experimental import pallas as pl
from jax.experimental.pallas import tpu as pltpu
from jax.sharding import Mesh
from jax.sharding import PartitionSpec as P


NOPE = 128
ROPE = 64
VDIM = 128
WIDE = 256
SUB = 128
HALO = 256
SEQ = ("z", "y")
GROUP = ("x", "c")
EVERY = ("z", "y", "x", "c")
CHUNK = 640
STRIP = 16
VMEM_LIMIT = 24 * 2**20
INTERPRET = False
LOWEST = -1e30


def spread(value, axis):
    count = lax.axis_size(axis)
    copies = jnp.broadcast_to(value[None], (count, *value.shape))
    return lax.all_to_all(copies, axis, 0, 0)


def shifted(value, axes, steps):
    count = lax.axis_size(axes)
    return lax.ppermute(value, axes, [(i, i + steps) for i in range(count - steps)])


def turned(value, axis, steps):
    count = lax.axis_size(axis)
    return lax.ppermute(value, axis, [(i, (i + steps) % count) for i in range(count)])


def swapped(value):
    return lax.ppermute(value, "c", [(0, 1), (1, 0)])


def hops(step, flip):
    chips = lax.axis_size("x")
    return [
        (2 * x + c, 2 * ((x + step) % chips) + (c ^ flip)) for x in range(chips) for c in range(2)
    ]


def project_kernel(weight_rows, places, chips, at_ref, mine_ref, other_ref, *refs):
    weights, (k_ref, v_ref, w_ref, l_ref) = iter(refs[:-4]), refs[-4:]
    over_y = len(places)
    for step, parts in places:
        at_y = lax.rem(at_ref[1] + over_y - step, over_y)
        z = 0
        for _ in range(parts):
            piece = next(weights)
            for row in range(0, piece.shape[0], weight_rows):
                at = pl.multiple_of((z * over_y + at_y) * weight_rows, weight_rows)
                w_ref[pl.ds(at, weight_rows), :] = piece[row : row + weight_rows, :]
                z += 1
    rank = w_ref.shape[0]
    cols = v_ref.shape[1]
    for part, core in ((mine_ref, at_ref[2]), (other_ref, 1 - at_ref[2])):
        for i in range(part.shape[0] // SUB):
            chip = lax.rem(at_ref[0] + chips - i, chips) if i < chips else i - chips
            first = HALO if i < chips else 0
            at = pl.multiple_of(first + (2 * chip + core) * SUB, SUB)
            l_ref[pl.ds(at, SUB), :] = part[i * SUB : (i + 1) * SUB, :]

    for at in range(0, l_ref.shape[0], CHUNK):
        rows = slice(at, at + CHUNK)
        rope = l_ref[rows, rank:].astype(jnp.float32)
        rope_high = pltpu.roll(rope, ROPE, 1)
        low = lax.broadcasted_iota(jnp.int32, rope.shape, 1) < ROPE
        for col in range(0, 2 * cols, 256):
            product = jnp.dot(
                l_ref[rows, :rank], w_ref[:, col : col + 256], preferred_element_type=jnp.float32
            )
            if col >= cols:
                v_ref[rows, col - cols : col - cols + 256] = product.astype(jnp.bfloat16)
                continue
            moved = pltpu.roll(product[:, NOPE:], ROPE, 1)
            out = 2 * col
            k_ref[rows, out : out + 128] = product[:, :NOPE].astype(jnp.bfloat16)
            k_ref[rows, out + 128 : out + 256] = l_ref[rows, rank:]
            k_ref[rows, out + 256 : out + 384] = jnp.where(low, 0.0, moved).astype(jnp.bfloat16)
            k_ref[rows, out + 384 : out + 512] = jnp.where(low, moved, rope_high).astype(
                jnp.bfloat16
            )


IN_VMEM = pl.BlockSpec(memory_space=pltpu.VMEM)
IN_SMEM = pl.BlockSpec(memory_space=pltpu.SMEM)


def joined_kernel(*refs):
    *parts, out_ref = refs
    at = 0
    for part in parts:
        out_ref[at : at + part.shape[0], :] = part[...]
        at += part.shape[0]


def joined(parts):
    rows = sum(part.shape[0] for part in parts)
    return pl.pallas_call(
        joined_kernel,
        in_specs=[IN_VMEM] * len(parts),
        out_specs=IN_VMEM,
        out_shape=jax.ShapeDtypeStruct((rows, parts[0].shape[1]), parts[0].dtype),
        compiler_params=pltpu.CompilerParams(vmem_limit_bytes=VMEM_LIMIT),
        cost_estimate=pl.CostEstimate(
            flops=rows * 1024, bytes_accessed=rows * 2560, transcendentals=0
        ),
        interpret=INTERPRET,
        name="joined",
    )(*parts)


def project(mine, other, weights):
    chips = lax.axis_size("x")
    rows = mine.shape[0] * 2
    places = tuple((step, len(parts)) for step, *parts in weights)
    weights = [part for _, *parts in weights for part in parts]
    cols = weights[0].shape[1] // 2
    rank = weights[0].shape[0] * len(places)
    at = jnp.stack([lax.axis_index(axis) for axis in ("x", "y", "c")]).astype(jnp.int32)
    weight_rows = weights[0].shape[0] // lax.axis_size("z")
    return pl.pallas_call(
        functools.partial(project_kernel, weight_rows, places, chips),
        in_specs=[IN_SMEM] + [IN_VMEM] * (2 + len(weights)),
        out_specs=[IN_VMEM, IN_VMEM],
        scratch_shapes=[
            pltpu.VMEM((rank, 2 * cols), jnp.bfloat16),
            pltpu.VMEM((rows, mine.shape[1]), jnp.bfloat16),
        ],
        out_shape=[
            jax.ShapeDtypeStruct((rows, 2 * cols), jnp.bfloat16),
            jax.ShapeDtypeStruct((rows, cols), jnp.bfloat16),
        ],
        compiler_params=pltpu.CompilerParams(vmem_limit_bytes=VMEM_LIMIT),
        cost_estimate=pl.CostEstimate(
            flops=4 * rows * rank * cols, bytes_accessed=8 * rows * cols, transcendentals=0
        ),
        interpret=INTERPRET,
        name="project",
    )(at, mine, other, *weights)


def attend_kernel(
    score_scale, at_ref, q0_ref, q1_ref, k_ref, v_ref, start_ref, o0_ref, o1_ref, *scratch
):
    q_ref, o_ref, bias_ref, s_ref, p_ref, t_ref = scratch
    rows, window = 2 * SUB, 2 * SUB + HALO
    heads = v_ref.shape[1] // VDIM
    base = pl.multiple_of(at_ref[0], 2 * SUB)
    places = [pl.ds(pl.multiple_of(at_ref[1 + i], SUB), SUB) for i in range(2)]
    q_ref[places[0], :] = q0_ref[...]
    q_ref[places[1], :] = q1_ref[...]
    for at in range(0, rows, STRIP):
        row = lax.broadcasted_iota(jnp.int32, (STRIP, window), 0) + at
        col = lax.broadcasted_iota(jnp.int32, (STRIP, window), 1)
        start = start_ref[pl.ds(pl.multiple_of(base + at, STRIP), STRIP), :] - base
        allowed = (col <= row + HALO) & (col >= start)
        bias_ref[at : at + STRIP, :] = jnp.where(allowed, 0.0, LOWEST)
    span = pl.ds(base, window)

    @pl.loop(0, heads // 2)
    def _(pair):
        for half in range(2):
            q_at = pl.multiple_of(pair * 2 * (NOPE + ROPE) + 128 * half, 128)
            v_at = pl.ds(pl.multiple_of((2 * pair + half) * VDIM, VDIM), VDIM)
            k_at = pl.ds(pl.multiple_of((2 * pair + half) * WIDE, WIDE), WIDE)
            s_ref[half] = lax.dot_general(
                q_ref[:, pl.ds(q_at, WIDE)],
                k_ref[span, k_at],
                (((1,), (1,)), ((), ())),
                preferred_element_type=jnp.float32,
            )
        for half in range(2):
            v_at = pl.ds(pl.multiple_of((2 * pair + half) * VDIM, VDIM), VDIM)
            for at in range(0, rows, STRIP):
                part = slice(at, at + STRIP)
                scores = s_ref[half, part, :] * score_scale + bias_ref[part, :]
                expo = jnp.exp2(scores - jnp.max(scores, axis=1, keepdims=True))
                t_ref[half, part, :] = jnp.broadcast_to(
                    jnp.sum(expo, axis=1, keepdims=True), (STRIP, VDIM)
                )
                p_ref[half, part, :] = expo.astype(jnp.bfloat16)
            mixed = jnp.dot(p_ref[half], v_ref[span, v_at], preferred_element_type=jnp.float32)
            o_ref[:, v_at] = (mixed / t_ref[half]).astype(jnp.bfloat16)

    o0_ref[...] = o_ref[places[0], :]
    o1_ref[...] = o_ref[places[1], :]


def attend(chip, mine, other, keys, values, starts):
    rows, width = mine.shape
    heads = values.shape[1] // VDIM
    window = 2 * SUB + HALO
    core = lax.axis_index("c")
    at = jnp.stack([chip * 2 * SUB, core * SUB, (1 - core) * SUB]).astype(jnp.int32)
    score_scale = math.log2(math.e) / math.sqrt(NOPE + ROPE)
    o_shape = jax.ShapeDtypeStruct((rows, heads * VDIM), jnp.bfloat16)
    return pl.pallas_call(
        functools.partial(attend_kernel, score_scale),
        in_specs=[IN_SMEM] + [IN_VMEM] * 5,
        out_specs=[IN_VMEM, IN_VMEM],
        out_shape=[o_shape, o_shape],
        scratch_shapes=[
            pltpu.VMEM((2 * SUB, width), jnp.bfloat16),
            pltpu.VMEM((2 * SUB, heads * VDIM), jnp.bfloat16),
            pltpu.VMEM((2 * SUB, window), jnp.float32),
            pltpu.VMEM((2, 2 * SUB, window), jnp.float32),
            pltpu.VMEM((2, 2 * SUB, window), jnp.bfloat16),
            pltpu.VMEM((2, 2 * SUB, VDIM), jnp.float32),
        ],
        compiler_params=pltpu.CompilerParams(vmem_limit_bytes=VMEM_LIMIT),
        cost_estimate=pl.CostEstimate(
            flops=40 * heads * rows * window * (WIDE + VDIM),
            bytes_accessed=4 * rows * heads * 1024,
            transcendentals=2 * heads * rows * window,
        ),
        interpret=INTERPRET,
        name="attend",
    )(at, mine, other, keys, values, starts)


def whole(queries, latent, rope_keys, key_weight, value_weight, doc_lengths):
    tok_rows, _ = latent.shape
    chips = lax.axis_size("x")
    groups = 2 * chips
    group_rows = tok_rows * groups
    width = queries.shape[1] // groups
    x, core = lax.axis_index("x"), lax.axis_index("c")

    def block_of(step, flip):
        return 2 * lax.rem(x + step, chips) + (core ^ flip)

    weights = jnp.concatenate([key_weight, value_weight], axis=1)
    weights = spread(weights, "z").reshape(-1, weights.shape[1])
    over_y = lax.axis_size("y")
    weight_pieces = [(s, turned(weights, "y", s) if s else weights) for s in range(over_y)]

    both = jnp.concatenate(
        [latent, rope_keys, jnp.zeros((tok_rows, 128 - ROPE), jnp.bfloat16)], axis=1
    )
    parts = [both] + [turned(both, "x", s) for s in range(1, chips)]
    halo_chips = HALO // (2 * tok_rows)
    last = []
    for chip in range(chips - halo_chips, chips):
        behind = lax.rem(x + chips - chip, chips)
        last.append(lax.select_n(behind, *parts))
    last = jnp.concatenate(last, axis=0)
    earlier = shifted(last, SEQ, 1)
    mine = joined([*parts, earlier])
    other = swapped(mine)

    late, _ = lax.optimization_barrier((queries, last))

    def sent(step, flip):
        out = lax.dynamic_slice_in_dim(queries if step % 2 else late, width * block_of(step, flip), width, 1)
        if not (step or flip):
            return out
        return lax.ppermute(out, GROUP, hops(step, flip))

    arrived = {(s, f): sent(s, f) for s in range(chips) for f in (0, 1)}

    docs = doc_lengths.shape[0]
    earlier = jnp.arange(docs)[None, :] < jnp.arange(docs)[:, None]
    starts = jnp.sum(jnp.where(earlier, doc_lengths[None, :], 0), axis=1)
    first_place = lax.axis_index(SEQ) * group_rows
    places = first_place + jnp.arange(group_rows, dtype=jnp.int32)
    own = jnp.max(
        jnp.where(starts[None, :] <= places[:, None], starts[None, :], 0), axis=1, keepdims=True
    )
    own = (own - first_place + HALO).astype(jnp.int32)

    keys, values = project(mine, other, weight_pieces)

    result = jnp.zeros((tok_rows, groups * value_weight.shape[1]), jnp.bfloat16)
    for step in (2, 1, 3, 0):
        chip = lax.rem(x + chips - step, chips)
        pair = attend(chip, arrived[step, 0], arrived[step, 1], keys, values, own)
        for flip in (0, 1):
            back = pair[flip]
            if step or flip:
                back = lax.ppermute(back, GROUP, [(b, a) for a, b in hops(step, flip)])
            at = value_weight.shape[1] * block_of(step, flip)
            result = lax.dynamic_update_slice(result, back, (0, at))
    return result


def solution(mesh):
    y = 4 if mesh.shape["seq"] % 4 == 0 else 1
    torus = Mesh(mesh.devices.reshape(-1, y, mesh.shape["head"] // 2, 2), EVERY)
    in_specs = (
        P(EVERY, None),
        P(EVERY, None),
        P(EVERY, None),
        P(SEQ, GROUP),
        P(SEQ, GROUP),
        P(),
    )
    return jax.shard_map(
        whole, mesh=torus, in_specs=in_specs, out_specs=P(EVERY, None), check_vma=False
    )
```

```python
import functools
import math

import jax
import jax.numpy as jnp
from jax import lax
from jax.experimental import pallas as pl
from jax.experimental.pallas import tpu as pltpu
from jax.sharding import Mesh
from jax.sharding import PartitionSpec as P


NOPE = 128
ROPE = 64
VDIM = 128
WIDE = 256
SUB = 128
HALO = 256
SEQ = ("z", "y")
GROUP = ("x", "c")
EVERY = ("z", "y", "x", "c")
CHUNK = 640
TOGETHER = 8
STRIP = 16
VMEM_LIMIT = 24 * 2**20
INTERPRET = False
LOWEST = -1e30


def spread(value, axis):
    count = lax.axis_size(axis)
    copies = jnp.broadcast_to(value[None], (count, *value.shape))
    return lax.all_to_all(copies, axis, 0, 0)


def shifted(value, axes, steps):
    count = lax.axis_size(axes)
    return lax.ppermute(value, axes, [(i, i + steps) for i in range(count - steps)])


def turned(value, axis, steps):
    count = lax.axis_size(axis)
    return lax.ppermute(value, axis, [(i, (i + steps) % count) for i in range(count)])


def swapped(value):
    return lax.ppermute(value, "c", [(0, 1), (1, 0)])


def hops(step, flip):
    chips = lax.axis_size("x")
    return [
        (2 * x + c, 2 * ((x + step) % chips) + (c ^ flip)) for x in range(chips) for c in range(2)
    ]


def project_kernel(weight_rows, places, chips, at_ref, mine_ref, other_ref, *refs):
    weights, (k_ref, v_ref, w_ref, l_ref) = iter(refs[:-4]), refs[-4:]
    over_y = len(places)
    for step, parts in places:
        at_y = lax.rem(at_ref[1] + over_y - step, over_y)
        z = 0
        for _ in range(parts):
            piece = next(weights)
            for row in range(0, piece.shape[0], weight_rows):
                at = pl.multiple_of((z * over_y + at_y) * weight_rows, weight_rows)
                w_ref[pl.ds(at, weight_rows), :] = piece[row : row + weight_rows, :]
                z += 1
    rank = w_ref.shape[0]
    cols = v_ref.shape[1]
    for part, core in ((mine_ref, at_ref[2]), (other_ref, 1 - at_ref[2])):
        for i in range(part.shape[0] // SUB):
            chip = lax.rem(at_ref[0] + chips - i, chips) if i < chips else i - chips
            first = HALO if i < chips else 0
            at = pl.multiple_of(first + (2 * chip + core) * SUB, SUB)
            l_ref[pl.ds(at, SUB), :] = part[i * SUB : (i + 1) * SUB, :]

    for at in range(0, l_ref.shape[0], CHUNK):
        rows = slice(at, at + CHUNK)
        rope = l_ref[rows, rank:].astype(jnp.float32)
        rope_high = pltpu.roll(rope, ROPE, 1)
        low = lax.broadcasted_iota(jnp.int32, rope.shape, 1) < ROPE
        for col in range(0, 2 * cols, 256):
            product = jnp.dot(
                l_ref[rows, :rank], w_ref[:, col : col + 256], preferred_element_type=jnp.float32
            )
            if col >= cols:
                v_ref[rows, col - cols : col - cols + 256] = product.astype(jnp.bfloat16)
                continue
            moved = pltpu.roll(product[:, NOPE:], ROPE, 1)
            out = 2 * col
            k_ref[rows, out : out + 128] = product[:, :NOPE].astype(jnp.bfloat16)
            k_ref[rows, out + 128 : out + 256] = l_ref[rows, rank:]
            k_ref[rows, out + 256 : out + 384] = jnp.where(low, 0.0, moved).astype(jnp.bfloat16)
            k_ref[rows, out + 384 : out + 512] = jnp.where(low, moved, rope_high).astype(
                jnp.bfloat16
            )


IN_VMEM = pl.BlockSpec(memory_space=pltpu.VMEM)
IN_SMEM = pl.BlockSpec(memory_space=pltpu.SMEM)


def joined_kernel(*refs):
    *parts, out_ref = refs
    at = 0
    for part in parts:
        out_ref[at : at + part.shape[0], :] = part[...]
        at += part.shape[0]


def joined(parts):
    rows = sum(part.shape[0] for part in parts)
    return pl.pallas_call(
        joined_kernel,
        in_specs=[IN_VMEM] * len(parts),
        out_specs=IN_VMEM,
        out_shape=jax.ShapeDtypeStruct((rows, parts[0].shape[1]), parts[0].dtype),
        compiler_params=pltpu.CompilerParams(vmem_limit_bytes=VMEM_LIMIT),
        cost_estimate=pl.CostEstimate(
            flops=rows * 1024, bytes_accessed=rows * 2560, transcendentals=0
        ),
        interpret=INTERPRET,
        name="joined",
    )(*parts)


def project(mine, other, weights):
    chips = lax.axis_size("x")
    rows = mine.shape[0] * 2
    places = tuple((step, len(parts)) for step, *parts in weights)
    weights = [part for _, *parts in weights for part in parts]
    cols = weights[0].shape[1] // 2
    rank = weights[0].shape[0] * len(places)
    at = jnp.stack([lax.axis_index(axis) for axis in ("x", "y", "c")]).astype(jnp.int32)
    weight_rows = weights[0].shape[0] // lax.axis_size("z")
    return pl.pallas_call(
        functools.partial(project_kernel, weight_rows, places, chips),
        in_specs=[IN_SMEM] + [IN_VMEM] * (2 + len(weights)),
        out_specs=[IN_VMEM, IN_VMEM],
        scratch_shapes=[
            pltpu.VMEM((rank, 2 * cols), jnp.bfloat16),
            pltpu.VMEM((rows, mine.shape[1]), jnp.bfloat16),
        ],
        out_shape=[
            jax.ShapeDtypeStruct((rows, 2 * cols), jnp.bfloat16),
            jax.ShapeDtypeStruct((rows, cols), jnp.bfloat16),
        ],
        compiler_params=pltpu.CompilerParams(vmem_limit_bytes=VMEM_LIMIT),
        cost_estimate=pl.CostEstimate(
            flops=4 * rows * rank * cols, bytes_accessed=8 * rows * cols, transcendentals=0
        ),
        interpret=INTERPRET,
        name="project",
    )(at, mine, other, *weights)


def attend_kernel(
    score_scale, at_ref, q0_ref, q1_ref, k_ref, v_ref, start_ref, o0_ref, o1_ref, *scratch
):
    q_ref, o_ref, bias_ref, s_ref, p_ref, t_ref = scratch
    rows, window = 2 * SUB, 2 * SUB + HALO
    heads = v_ref.shape[1] // VDIM
    base = pl.multiple_of(at_ref[0], 2 * SUB)
    places = [pl.ds(pl.multiple_of(at_ref[1 + i], SUB), SUB) for i in range(2)]
    q_ref[places[0], :] = q0_ref[...]
    q_ref[places[1], :] = q1_ref[...]
    for at in range(0, rows, STRIP):
        row = lax.broadcasted_iota(jnp.int32, (STRIP, window), 0) + at
        col = lax.broadcasted_iota(jnp.int32, (STRIP, window), 1)
        start = start_ref[pl.ds(pl.multiple_of(base + at, STRIP), STRIP), :] - base
        allowed = (col <= row + HALO) & (col >= start)
        bias_ref[at : at + STRIP, :] = jnp.where(allowed, 0.0, LOWEST)
    span = pl.ds(base, window)

    @pl.loop(0, heads // TOGETHER)
    def _(turn):
        for half in range(TOGETHER):
            q_at = (turn * TOGETHER + half // 2 * 2) * (NOPE + ROPE) + 128 * (half % 2)
            q_at = pl.multiple_of(q_at, 128)
            k_at = pl.ds(pl.multiple_of((TOGETHER * turn + half) * WIDE, WIDE), WIDE)
            s_ref[half] = lax.dot_general(
                q_ref[:, pl.ds(q_at, WIDE)],
                k_ref[span, k_at],
                (((1,), (1,)), ((), ())),
                preferred_element_type=jnp.float32,
            )
        for half in range(TOGETHER):
            v_at = pl.ds(pl.multiple_of((TOGETHER * turn + half) * VDIM, VDIM), VDIM)
            for at in range(0, rows, STRIP):
                part = slice(at, at + STRIP)
                scores = s_ref[half, part, :] * score_scale + bias_ref[part, :]
                expo = jnp.exp2(scores - jnp.max(scores, axis=1, keepdims=True))
                t_ref[half, part, :] = jnp.broadcast_to(
                    jnp.sum(expo, axis=1, keepdims=True), (STRIP, VDIM)
                )
                p_ref[half, part, :] = expo.astype(jnp.bfloat16)
            mixed = jnp.dot(p_ref[half], v_ref[span, v_at], preferred_element_type=jnp.float32)
            o_ref[:, v_at] = (mixed / t_ref[half]).astype(jnp.bfloat16)

    o0_ref[...] = o_ref[places[0], :]
    o1_ref[...] = o_ref[places[1], :]


def attend(chip, mine, other, keys, values, starts):
    rows, width = mine.shape
    heads = values.shape[1] // VDIM
    window = 2 * SUB + HALO
    core = lax.axis_index("c")
    at = jnp.stack([chip * 2 * SUB, core * SUB, (1 - core) * SUB]).astype(jnp.int32)
    score_scale = math.log2(math.e) / math.sqrt(NOPE + ROPE)
    o_shape = jax.ShapeDtypeStruct((rows, heads * VDIM), jnp.bfloat16)
    return pl.pallas_call(
        functools.partial(attend_kernel, score_scale),
        in_specs=[IN_SMEM] + [IN_VMEM] * 5,
        out_specs=[IN_VMEM, IN_VMEM],
        out_shape=[o_shape, o_shape],
        scratch_shapes=[
            pltpu.VMEM((2 * SUB, width), jnp.bfloat16),
            pltpu.VMEM((2 * SUB, heads * VDIM), jnp.bfloat16),
            pltpu.VMEM((2 * SUB, window), jnp.float32),
            pltpu.VMEM((TOGETHER, 2 * SUB, window), jnp.float32),
            pltpu.VMEM((TOGETHER, 2 * SUB, window), jnp.bfloat16),
            pltpu.VMEM((TOGETHER, 2 * SUB, VDIM), jnp.float32),
        ],
        compiler_params=pltpu.CompilerParams(vmem_limit_bytes=VMEM_LIMIT),
        cost_estimate=pl.CostEstimate(
            flops=40 * heads * rows * window * (WIDE + VDIM),
            bytes_accessed=4 * rows * heads * 1024,
            transcendentals=2 * heads * rows * window,
        ),
        interpret=INTERPRET,
        name="attend",
    )(at, mine, other, keys, values, starts)


def whole(queries, latent, rope_keys, key_weight, value_weight, doc_lengths):
    tok_rows, _ = latent.shape
    chips = lax.axis_size("x")
    groups = 2 * chips
    group_rows = tok_rows * groups
    width = queries.shape[1] // groups
    x, core = lax.axis_index("x"), lax.axis_index("c")

    def block_of(step, flip):
        return 2 * lax.rem(x + step, chips) + (core ^ flip)

    weights = jnp.concatenate([key_weight, value_weight], axis=1)
    weights = spread(weights, "z").reshape(-1, weights.shape[1])
    over_y = lax.axis_size("y")
    weight_pieces = [(s, turned(weights, "y", s) if s else weights) for s in range(over_y)]

    both = jnp.concatenate(
        [latent, rope_keys, jnp.zeros((tok_rows, 128 - ROPE), jnp.bfloat16)], axis=1
    )
    parts = [both] + [turned(both, "x", s) for s in range(1, chips)]
    halo_chips = HALO // (2 * tok_rows)
    last = []
    for chip in range(chips - halo_chips, chips):
        behind = lax.rem(x + chips - chip, chips)
        last.append(lax.select_n(behind, *parts))
    last = jnp.concatenate(last, axis=0)
    earlier = shifted(last, SEQ, 1)
    mine = joined([*parts, earlier])
    other = swapped(mine)

    late, _ = lax.optimization_barrier((queries, last))

    def sent(step, flip):
        out = lax.dynamic_slice_in_dim(queries if step % 2 else late, width * block_of(step, flip), width, 1)
        if not (step or flip):
            return out
        return lax.ppermute(out, GROUP, hops(step, flip))

    arrived = {(s, f): sent(s, f) for s in range(chips) for f in (0, 1)}

    docs = doc_lengths.shape[0]
    earlier = jnp.arange(docs)[None, :] < jnp.arange(docs)[:, None]
    starts = jnp.sum(jnp.where(earlier, doc_lengths[None, :], 0), axis=1)
    first_place = lax.axis_index(SEQ) * group_rows
    places = first_place + jnp.arange(group_rows, dtype=jnp.int32)
    own = jnp.max(
        jnp.where(starts[None, :] <= places[:, None], starts[None, :], 0), axis=1, keepdims=True
    )
    own = (own - first_place + HALO).astype(jnp.int32)

    keys, values = project(mine, other, weight_pieces)

    result = jnp.zeros((tok_rows, groups * value_weight.shape[1]), jnp.bfloat16)
    for step in (2, 1, 3, 0):
        chip = lax.rem(x + chips - step, chips)
        pair = attend(chip, arrived[step, 0], arrived[step, 1], keys, values, own)
        for flip in (0, 1):
            back = pair[flip]
            if step or flip:
                back = lax.ppermute(back, GROUP, [(b, a) for a, b in hops(step, flip)])
            at = value_weight.shape[1] * block_of(step, flip)
            result = lax.dynamic_update_slice(result, back, (0, at))
    return result


def solution(mesh):
    y = 4 if mesh.shape["seq"] % 4 == 0 else 1
    torus = Mesh(mesh.devices.reshape(-1, y, mesh.shape["head"] // 2, 2), EVERY)
    in_specs = (
        P(EVERY, None),
        P(EVERY, None),
        P(EVERY, None),
        P(SEQ, GROUP),
        P(SEQ, GROUP),
        P(),
    )
    return jax.shard_map(
        whole, mesh=torus, in_specs=in_specs, out_specs=P(EVERY, None), check_vma=False
    )
```
